32 devices in a mesh: groups: 2 (over y), dp: 2 (over core), tensor: 8 (over z, x).
Axes of the slice: x: 2, y: 2, z: 4, core: 2. Of those that a mesh axis runs over, the one named last changes fastest.
Arguments:
- hidden_in: bfloat16 [4, 1024, 5120], P(('groups', 'dp'), 'tensor'), parts along dimension 0, may hold values from -40 to 40
- first_values: bfloat16 [4, 1024, 1024], P(('groups', 'dp'), 'tensor'), parts along dimension 0, may hold values from -6 to 6
- qkv_weight: bfloat16 [5120, 3, 1024], P(None, None, 'tensor'), may hold values from -1 to 1
- out_weight: bfloat16 [1024, 5120], P('tensor'), may hold values from -0.1875 to 0.1875
- mix_table: float32 [8, 2], replicated, may hold values from 0.2 to 1
- mix_index: int32 [8], P('tensor'), may hold values from 0 to 7
- lengths: int32 [4], P(('groups', 'dp')), parts along dimension 0, may hold values from 256 to 1024
Outputs:
- attn_out: bfloat16 [4, 1024, 5120], P(('groups', 'dp'), 'tensor'), parts along dimension 0
The draws below stay inside these ranges and needn't reach their ends.
There are 2 independent parts, one for each index of `groups`. The reference program is written for one: setup_inputs(seed, part) draws one part's arguments, and reference() takes and returns one part's arrays. A program takes and returns all parts, laid end to end along the dimension named above; an argument that names none is the same for every part. Nothing has to cross between parts.
All inputs are finite; a program needn't handle non-finite values.
Results may differ from the reference program's by a relative error of at most 0.0077.
Values may be sent and summed in bfloat16 or wider, within the bound.
A program may use at most 128 MiB of HBM per device.

```python
import math
import jax
import jax.numpy as jnp
from jax import lax

D = 5120
HS = 128
MIXES = 8
SEQ = 1024
HEADS = 8
SEQS = 2


def draw_hidden_in(key, part):
    samples = jnp.clip(jax.random.normal(jax.random.fold_in(key, 11), (SEQS, SEQ, D), jnp.float32), -6.0, 6.0)
    return samples.astype(jnp.bfloat16)


def draw_qkv_weight(key, part):
    inner_width = HEADS * HS
    spread = 1.0 / math.sqrt(D)
    weights = jax.random.normal(jax.random.fold_in(key, 21), (D, 3, inner_width), jnp.float32) * spread
    return jnp.clip(weights, -1.0, 1.0).astype(jnp.bfloat16)


def with_ends(drawn, own_key, least, top_value):
    longest = drawn.shape.index(max(drawn.shape))
    spots = []
    for shift in (0, 1):
        where = [jax.random.randint(jax.random.fold_in(own_key, axis), (), 0, length) for axis, length in enumerate(drawn.shape)]
        where[longest] = (where[longest] + shift) % drawn.shape[longest]
        spots.append(tuple(where))
    return drawn.at[spots[0]].set(least).at[spots[1]].set(top_value)


def level_of(key, dims, cuts, smallest, high):
    gain, own = 1.0, jax.random.fold_in(key, 6)
    for position, shards_of in cuts:
        steps = jnp.exp(jax.random.uniform(jax.random.fold_in(own, position), (shards_of,), jnp.float32, smallest / len(cuts), high / len(cuts)))
        gain = gain * jnp.repeat(steps, dims[position] // shards_of).reshape([-1 if axis == position else 1 for axis in range(len(dims))])
    return gain


def scatter_about(stream_key, dims, width, limit, shards=(), kind=jnp.bfloat16):
    values = width * jax.random.normal(stream_key, dims, jnp.float32)
    if shards:
        values = values * level_of(stream_key, dims, shards, -0.22, 0.18)
    return jnp.clip(values, -limit, limit).astype(kind)


def setup_inputs(seed: int = 0, part: int = 0) -> dict:
    splits = jax.random.split(jax.random.key(seed), 8)
    own_keys = jax.random.split(jax.random.fold_in(splits[7], part), 8)
    hidden_in = draw_hidden_in(jax.random.fold_in(jax.random.fold_in(splits[7], part), 71), part)
    first_values = scatter_about(own_keys[1], (SEQS, SEQ, HEADS * HS), 1.0, 6.0, ((0, 2), (1, 8)))
    qkv_weight = draw_qkv_weight(jax.random.fold_in(splits[7], 71), part)
    out_weight = scatter_about(splits[3], (HEADS * HS, D), (8 * HS) ** -0.5, 0.1875, ((0, 8),))
    mix_table = jnp.clip(jax.random.uniform(splits[4], (MIXES, 2), jnp.float32, 0.2, 1.0), 0.2, 1.0)
    mix_index = with_ends(jax.random.randint(splits[5], (HEADS,), 0, MIXES), jax.random.fold_in(splits[5], 1), 0, MIXES - 1).astype(jnp.int32)
    lengths = jax.random.randint(own_keys[6], (SEQS,), SEQ // 4, SEQ + 1).astype(jnp.int32)
    return {"hidden_in": hidden_in, "first_values": first_values, "qkv_weight": qkv_weight, "out_weight": out_weight, "mix_table": mix_table, "mix_index": mix_index, "lengths": lengths}


NEG_FILL = -1e+30

def reference(hidden_in, first_values, qkv_weight, out_weight, mix_table, mix_index, lengths):
    merged_weight = qkv_weight.reshape(D, 3 * HEADS * HS)
    lambdas = mix_table[mix_index]
    score_scale = 1.0 / math.sqrt(HS)
    positions = jnp.arange(SEQ, dtype=jnp.int32)

    def one_sequence(packed):
        tok_rows, firsts, valid_length = packed
        projected = jnp.dot(tok_rows, merged_weight, preferred_element_type=jnp.float32).astype(jnp.bfloat16)
        split_parts = projected.reshape(SEQ, 3, HEADS, HS)
        first_float = firsts.reshape(SEQ, HEADS, HS).astype(jnp.float32)
        value_float = split_parts[:, 2].astype(jnp.float32)
        mixed_values = (lambdas[None, :, 0:1] * value_float + lambdas[None, :, 1:2] * first_float).astype(jnp.bfloat16)
        allowed = (positions[None, :] <= positions[:, None]) & (positions[None, :] < valid_length)

        def one_head(items):
            query_rows, key_rows, value_rows = items
            scores = jnp.dot(query_rows, key_rows.T, preferred_element_type=jnp.float32) * score_scale
            scores = jnp.where(allowed, scores, NEG_FILL)
            row_max = lax.optimization_barrier(jnp.max(scores, axis=1, keepdims=True))
            raised = jnp.exp(scores - row_max)
            weights = (raised / lax.optimization_barrier(jnp.sum(raised, axis=1, keepdims=True))).astype(jnp.bfloat16)
            return jnp.dot(weights, value_rows, preferred_element_type=jnp.float32).astype(jnp.bfloat16)
        per_head = lax.map(one_head, (jnp.transpose(split_parts[:, 0], (1, 0, 2)), jnp.transpose(split_parts[:, 1], (1, 0, 2)), jnp.transpose(mixed_values, (1, 0, 2))))
        attended = jnp.transpose(per_head, (1, 0, 2)).reshape(SEQ, HEADS * HS)
        return jnp.dot(attended, out_weight, preferred_element_type=jnp.float32).astype(jnp.bfloat16)
    return lax.map(one_sequence, (hidden_in, first_values, lengths))
```

```python
import functools
import math

import jax
import jax.numpy as jnp
from jax import lax
from jax.experimental import pallas as pl
from jax.experimental.pallas import tpu as pltpu
from jax.sharding import PartitionSpec as P

NEG_FILL = -1e30
PAIR = 2


def attention(queries, key_rows, mixed_values, valid_length, head_size):
    total_rows = queries.shape[0]
    positions = jnp.arange(total_rows, dtype=jnp.int32)
    score_scale = 1.0 / math.sqrt(head_size)
    block_rows = min(512, total_rows)
    outputs = []
    for first_row in range(0, total_rows, block_rows):
        stop = first_row + block_rows
        scores = (
            jnp.einsum(
                "qhd,khd->hqk",
                queries[first_row:stop],
                key_rows[:stop],
                preferred_element_type=jnp.float32,
            )
            * score_scale
        )
        keys_at, rows_at = positions[:stop], positions[first_row:stop]
        allowed = (keys_at[None, :] <= rows_at[:, None]) & (keys_at[None, :] < valid_length)
        scores = jnp.where(allowed[None], scores, NEG_FILL)
        row_max = jnp.max(scores, axis=2, keepdims=True)
        raised = jnp.exp(scores - row_max)
        weights = (raised / jnp.sum(raised, axis=2, keepdims=True)).astype(jnp.bfloat16)
        outputs.append(
            jnp.einsum(
                "hqk,khd->qhd", weights, mixed_values[:stop], preferred_element_type=jnp.float32
            ).astype(jnp.bfloat16)
        )
    return jnp.concatenate(outputs, axis=0)


def body(hidden_in, first_values, qkv_weight, out_weight, mix_table, mix_index, lengths):
    local_rows = hidden_in[0]
    own_rows, model_width = local_rows.shape
    head_width = qkv_weight.shape[2]
    heads_here = mix_index.shape[0]
    head_size = head_width // heads_here
    ranks = lax.axis_size("tensor")
    cores = lax.axis_size("dp")
    rank = lax.axis_index("tensor")
    core = lax.axis_index("dp")
    side = rank % PAIR
    line = ranks // PAIR
    swap_pair = [(r, r ^ 1) for r in range(ranks)]
    swap_core = [(c, c ^ 1) for c in range(cores)]

    own_w = qkv_weight.reshape(model_width, 3 * head_width)
    half = model_width // 2
    sent = lax.dynamic_slice_in_dim(own_w, core * half, half, 0)
    got = lax.ppermute(sent, "tensor", swap_pair)
    got_other = lax.ppermute(got, "dp", swap_core)
    pair_w = jnp.where(
        core == 0,
        jnp.concatenate([got, got_other], axis=0),
        jnp.concatenate([got_other, got], axis=0),
    )

    lines = [[s + PAIR * i for i in range(line)] for s in range(PAIR)]
    rows = lax.all_gather(local_rows, "tensor", axis=0, tiled=True, axis_index_groups=lines)
    for_pair = jnp.dot(rows, pair_w, preferred_element_type=jnp.float32).astype(jnp.bfloat16)
    from_pair = lax.ppermute(for_pair, "tensor", swap_pair)
    ours = jnp.dot(rows, own_w, preferred_element_type=jnp.float32).astype(jnp.bfloat16)
    ours = ours.reshape(line, own_rows, 3 * head_width)
    from_pair = from_pair.reshape(line, own_rows, 3 * head_width)
    projected = jnp.where(
        side == 0,
        jnp.stack([ours, from_pair], axis=1),
        jnp.stack([from_pair, ours], axis=1),
    )
    total_rows = ranks * own_rows
    split_parts = projected.reshape(total_rows, 3, heads_here, head_size)

    relaid = lax.all_to_all(first_values[0], "tensor", split_axis=1, concat_axis=0, tiled=True)
    firsts = relaid.reshape(total_rows, heads_here, head_size)
    levels = mix_table.shape[0]
    one_hot = (mix_index[:, None] == jnp.arange(levels, dtype=jnp.int32)[None, :]).astype(
        jnp.float32
    )
    weights_mix = jnp.dot(one_hot, mix_table, precision=lax.Precision.HIGHEST)
    mixed_values = (
        weights_mix[None, :, 0:1] * split_parts[:, 2].astype(jnp.float32)
        + weights_mix[None, :, 1:2] * firsts.astype(jnp.float32)
    ).astype(jnp.bfloat16)
    attended = attention(
        split_parts[:, 0], split_parts[:, 1], mixed_values, lengths[0], head_size
    ).reshape(total_rows, head_width)

    gathered_bytes = ranks * out_weight.size * 2
    summed_bytes = total_rows * model_width * 4
    if gathered_bytes > summed_bytes:
        kept_rows = lax.psum_scatter(
            jnp.dot(attended, out_weight, preferred_element_type=jnp.float32),
            "tensor",
            scatter_dimension=0,
            tiled=True,
        )
        return kept_rows.astype(jnp.bfloat16)[None]

    part = head_width // 2
    own_part = lax.dynamic_slice_in_dim(out_weight, core * part, part, 0)
    mine = lax.all_gather(own_part, "tensor", axis=0, tiled=True)
    other = lax.ppermute(mine, "dp", swap_core)
    kept = lax.all_to_all(attended, "tensor", split_axis=0, concat_axis=1, tiled=True)
    kept = kept.reshape(own_rows, ranks, 2, part)
    low = kept[:, :, 0].reshape(own_rows, ranks * part)
    high = kept[:, :, 1].reshape(own_rows, ranks * part)
    out = jnp.dot(
        jnp.where(core == 0, low, high), mine, preferred_element_type=jnp.float32
    ) + jnp.dot(jnp.where(core == 0, high, low), other, preferred_element_type=jnp.float32)
    return out.astype(jnp.bfloat16)[None]


PIECES = 2
SHARERS = 4
BLOCKS = 4
MESH = pl.DeviceIdType.MESH


def whole_layer(
    line, rows_ref, w_ref, ow_ref, fv_ref, table_ref, index_ref, length_ref, out_ref,
    hid, wts, wf_ref, kept, px_out, px_in, finished, qkv_ref, fo_ref, att, gathered_att,
    load_sem, w_sem, wy_sem, wd_sem, we_sem, a1_sem, a2_sem, a3_sem, cx_sem, cz_sem,
    oz_sem, ox_sem, oy_sem, od_sem, oe_sem, fv_sem, at_sem,
):
    group, core, rank = lax.axis_index("groups"), lax.axis_index("dp"), lax.axis_index("tensor")
    spot, side = rank // PAIR, rank % PAIR
    ranks = line * PAIR
    steps = line - 1
    own_rows, width = rows_ref.shape
    half = width // PAIR
    part = half // SHARERS
    head = w_ref.shape[2]
    piece = own_rows // PIECES
    quarter = head // SHARERS
    mine, across = group * 2 + core, (1 - group) * 2 + core
    sib_mine, sib_across = group * 2 + 1 - core, (1 - group) * 2 + 1 - core
    near = spot + 1 - 2 * (spot % 2)
    far = (spot + line // 2) % line
    left, right = (group, core, rank - PAIR), (group, core, rank + PAIR)
    partner = (group, core, spot * PAIR + 1 - side)
    rows_peer = (group, core, far * PAIR + side)
    heads_peer = (group, core, near * PAIR + side)
    opposite = (1 - group, core, rank)
    sibling = (group, 1 - core, rank)
    has_left, has_right = spot > 0, spot < steps

    barrier = pltpu.get_barrier_semaphore()
    peers = [(group, core, (rank + o) % ranks) for o in range(1, ranks)]
    for there in peers + [opposite, sibling]:
        pl.semaphore_signal(barrier, inc=1, device_id=there, device_id_type=MESH)

    def cut(index, size):
        return pl.ds(pl.multiple_of(index * size, size), size)

    def row_block(b, p=None):
        if p is None:
            return pl.ds(b * own_rows, own_rows)
        return pl.ds(b * own_rows + p * piece, piece)

    own_half, other_half = cut(side, half), cut(1 - side, half)
    loads = [
        pltpu.make_async_copy(rows_ref.at[:, own_half], hid.at[row_block(0), :], load_sem.at[0]),
        pltpu.make_async_copy(w_ref.at[:, own_half, :], wts.at[0, :, :, pl.ds(0, head)], load_sem.at[1]),
        pltpu.make_async_copy(ow_ref, wf_ref.at[cut(rank, head), :], load_sem.at[2]),
        pltpu.make_async_copy(fv_ref.at[:, cut(rank, head)], fo_ref.at[cut(rank, own_rows), :], load_sem.at[3]),
    ]
    for load in loads:
        load.start()
    pl.semaphore_wait(barrier, ranks + 1)

    def send(src, dst, sems, at, there):
        return pltpu.make_async_remote_copy(
            src_ref=src, dst_ref=dst, send_sem=sems.at[(0,) + at], recv_sem=sems.at[(1,) + at],
            device_id=there, device_id_type=MESH,
        )

    def wpart(kind, j, q):
        zone, lane = (0, 1) if kind == 0 else (1, kind - 1)
        return wts.at[zone, j, cut(q, part), pl.ds(lane * head, head)]

    def w_source(s, j):
        return w_ref.at[j, pl.ds(pl.multiple_of(s * half + mine * part, part), part), :]

    def w_first(kind, j):
        if kind == 0:
            return send(w_source(1 - side, j), wpart(0, j, mine), w_sem, (0, j), partner)
        source = w_source(side, j) if kind == 1 else wpart(0, j, mine)
        return send(source, wpart(kind, j, mine), w_sem, (kind, j), heads_peer)

    def w_across(kind, j, q):
        return send(wpart(kind, j, q), wpart(kind, j, q), wy_sem, (kind, j), opposite)

    def w_down(kind, j, q):
        return send(wpart(kind, j, q), wpart(kind, j, q), wd_sem, (kind, j), sibling)

    def w_echo(kind, j, q):
        return send(wpart(kind, j, q), wpart(kind, j, q), we_sem, (kind, j), sibling)

    def arr(kind, j):
        w_first(kind, j).wait_recv()
        if kind == 0:
            w_first(2, j).start()
        w_across(kind, j, mine).start()
        w_down(kind, j, mine).start()

    def pas(kind, j):
        w_across(kind, j, across).wait_recv()
        w_echo(kind, j, across).start()

    def w_ready(kind):
        for j in range(3):
            w_down(kind, j, sib_mine).wait_recv()
            w_echo(kind, j, sib_across).wait_recv()

    def a1(p):
        return send(
            rows_ref.at[pl.ds(p * piece, piece), other_half], hid.at[row_block(1, p), :], a1_sem, (p,), partner
        )

    def a2(p):
        return send(
            rows_ref.at[pl.ds(p * piece, piece), own_half], hid.at[row_block(2, p), :], a2_sem, (p,), rows_peer
        )

    def a3(p):
        return send(hid.at[row_block(1, p), :], hid.at[row_block(3, p), :], a3_sem, (p,), rows_peer)

    def fwd(p):
        a1(p).wait_recv()
        a3(p).start()

    def swapped(b):
        return b + 1 - 2 * (b % 2)

    def cx(e, b):
        return pltpu.make_async_remote_copy(
            src_ref=px_out.at[e, b], dst_ref=px_in.at[e, swapped(b)], send_sem=cx_sem.at[0, e, b],
            recv_sem=cx_sem.at[1, e, swapped(b)], device_id=partner, device_id_type=MESH,
        )

    def place(b):
        return cut((spot, far)[b // 2] * PAIR + (side, 1 - side)[b % 2], own_rows)

    def cz(b):
        return send(finished.at[b], qkv_ref.at[:, place(b), :], cz_sem, (b,), heads_peer)

    def project(e, first, count):
        def one(j, carry):
            total = jnp.dot(
                hid[pl.ds(first * own_rows, count * own_rows), :], wts[e, j],
                preferred_element_type=jnp.float32,
            )
            for i in range(count):
                rows = total[i * own_rows : (i + 1) * own_rows]
                kept[e, first + i, j] = rows[:, :head]
                px_out[e, first + i, j] = rows[:, head:].astype(jnp.bfloat16)
            return carry

        lax.fori_loop(0, 3, one, 0)
        for b in range(first, first + count):
            cx(e, b).start()

    def comb(e, b):
        cx(e, swapped(b)).wait_recv()
        total = (kept[e, b] + px_in[e, b].astype(jnp.float32)).astype(jnp.bfloat16)
        if e == 0:
            qkv_ref[:, place(b), :] = total
        else:
            finished[b] = total
            cz(b).start()

    def first_copy(o):
        return send(fv_ref.at[:, cut(peers[o][2], head)], fo_ref.at[cut(rank, own_rows), :], fv_sem, (o,), peers[o])

    def wf(column, q):
        return wf_ref.at[pl.ds(pl.multiple_of(column * head + q * quarter, quarter), quarter), :]

    def wf_half(column, c):
        return wf_ref.at[pl.ds(pl.multiple_of(column * head + c * (head // 2), head // 2), head // 2), :]

    def chunk(way, k):
        return spot - 1 - k if way == 0 else spot + 1 + k

    def arrives(way, k):
        return k < spot if way == 0 else spot + 1 + k < line

    def leaves(way, k):
        if way == 0:
            return jnp.logical_and(k <= spot, has_right)
        return jnp.logical_and(spot + k < line, has_left)

    def carried(way, k):
        return spot - k if way == 0 else spot + k

    def column_of(kind, way, k):
        at = chunk(way, k)
        return at * PAIR + (side if kind == 0 else 1 - side)

    def out_z(way, k, at):
        column = at * PAIR + side
        source = ow_ref.at[cut(mine, quarter), :] if k == 0 else wf(column, mine)
        return send(source, wf(column, mine), oz_sem, (way, k), right if way == 0 else left)

    def out_x(way, k, column):
        return send(wf(column, mine), wf(column, mine), ox_sem, (way, k), partner)

    def out_y(kind, way, k, q):
        column = column_of(kind, way, k)
        return send(wf(column, q), wf(column, q), oy_sem, (kind, way, k), opposite)

    def out_d(kind, way, k, q):
        column = column_of(kind, way, k)
        return send(wf(column, q), wf(column, q), od_sem, (kind, way, k), sibling)

    def out_e(kind, way, k, q):
        column = column_of(kind, way, k)
        return send(wf(column, q), wf(column, q), oe_sem, (kind, way, k), sibling)

    partner_column = spot * PAIR + 1 - side

    def out_partner():
        return send(ow_ref.at[cut(core, head // 2), :], wf_half(rank, core), ox_sem, (2, 0), partner)

    def out_shared(c):
        return send(wf_half(partner_column, c), wf_half(partner_column, c), ox_sem, (2, 1), sibling)

    def oxp():
        out_partner().wait_recv()
        out_shared(core).start()

    def out_begin():
        for way in (0, 1):

            @pl.when(leaves(way, 0))
            def _():
                out_z(way, 0, spot).start()

    def oz(way, k):
        @pl.when(arrives(way, k))
        def _():
            at = chunk(way, k)
            out_z(way, k, at).wait_recv()
            if k + 1 < steps:

                @pl.when(leaves(way, k + 1))
                def _():
                    out_z(way, k + 1, at).start()

            out_x(way, k, column_of(0, way, k)).start()
            out_y(0, way, k, mine).start()
            out_d(0, way, k, mine).start()

    def ox(way, k):
        @pl.when(arrives(way, k))
        def _():
            out_x(way, k, column_of(1, way, k)).wait_recv()
            out_y(1, way, k, mine).start()
            out_d(1, way, k, mine).start()

    def oe(kind, way, k):
        @pl.when(arrives(way, k))
        def _():
            out_y(kind, way, k, across).wait_recv()
            out_e(kind, way, k, across).start()

    def begin_fv():
        for o in range(ranks - 1):
            first_copy(o).start()

    def near_dots():
        for load in loads:
            load.wait()
        w_ready(0)
        project(0, 0, 2)

    def far_dots():
        w_ready(1)
        w_ready(2)
        project(1, 0, 2)

    def row_dots(b, copy):
        for p in range(PIECES):
            copy(p).wait_recv()
        project(1, b, 1)
        project(0, b, 1)

    total_rows = ranks * own_rows
    block_rows = PAIR * own_rows

    def att_copy(o, r, me):
        return send(
            att.at[cut(r, own_rows), :], gathered_att.at[:, cut(me, head)], at_sem, (o,), peers[o]
        )

    def attend():
        for b in range(BLOCKS):
            cz(b).wait_recv()
        for o in range(ranks - 1):
            first_copy(o).wait_recv()
        chosen_row = index_ref[0]
        now, before = table_ref[0, chosen_row], table_ref[1, chosen_row]
        valid = length_ref[0]
        values = (now * qkv_ref[2].astype(jnp.float32) + before * fo_ref[...].astype(jnp.float32)).astype(
            jnp.bfloat16
        )
        score_scale = 1.0 / math.sqrt(head)
        for first_row in range(0, total_rows, block_rows):
            stop = first_row + block_rows
            scores = lax.dot_general(
                qkv_ref[0, first_row:stop, :], qkv_ref[1, :stop, :], (((1,), (1,)), ((), ())),
                preferred_element_type=jnp.float32,
            ) * score_scale
            shape = (block_rows, stop)
            limit = jnp.minimum(lax.broadcasted_iota(jnp.int32, (block_rows, 1), 0) + (first_row + 1), valid)
            scores = jnp.where(lax.broadcasted_iota(jnp.int32, shape, 1) < limit, scores, NEG_FILL)
            raised = jnp.exp(scores - jnp.max(scores, axis=1, keepdims=True))
            weights = (raised / jnp.sum(raised, axis=1, keepdims=True)).astype(jnp.bfloat16)
            att[first_row:stop, :] = jnp.dot(
                weights, values[:stop], preferred_element_type=jnp.float32
            ).astype(jnp.bfloat16)
        for o in range(ranks - 1):
            att_copy(o, peers[o][2], rank).start()
        own = pltpu.make_async_copy(
            att.at[cut(rank, own_rows), :], gathered_att.at[:, cut(rank, head)], load_sem.at[0]
        )
        own.start()
        own.wait()

    def each_column(action):
        for k in range(steps):
            for way in (0, 1):

                @pl.when(arrives(way, k))
                def _():
                    for kind in (0, 1):
                        action(kind, way, k)

    def column_in(kind, way, k):
        out_d(kind, way, k, sib_mine).wait_recv()
        out_e(kind, way, k, sib_across).wait_recv()

    def finish():
        for o in range(ranks - 1):
            att_copy(o, 0, (rank + ranks - 1 - o) % ranks).wait_recv()
        each_column(column_in)
        out_shared(1 - core).wait_recv()
        wide = width // (2 * PIECES * PAIR) if width % (1024 * PIECES) == 0 else width

        def one(i, carry):
            at = pl.ds(pl.multiple_of(i * wide, wide), wide)
            out_ref[:, at] = jnp.dot(
                gathered_att[...], wf_ref[:, at], preferred_element_type=jnp.float32
            ).astype(jnp.bfloat16)
            return carry

        lax.fori_loop(0, width // wide, one, 0)

    def drain():
        for p in range(PIECES):
            a1(p).wait_send()
            a2(p).wait_send()
            a3(p).wait_send()
        for kind in range(3):
            for j in range(3):
                w_first(kind, j).wait_send()
                w_across(kind, j, mine).wait_send()
                w_down(kind, j, mine).wait_send()
                w_echo(kind, j, across).wait_send()
        for e in range(2):
            for b in range(BLOCKS):
                cx(e, b).wait_send()
        for b in range(BLOCKS):
            cz(b).wait_send()
        for o in range(ranks - 1):
            first_copy(o).wait_send()
            att_copy(o, peers[o][2], rank).wait_send()
        out_partner().wait_send()
        out_shared(core).wait_send()

        def column_out(kind, way, k):
            if kind == 0:
                out_x(way, k, column_of(0, way, k)).wait_send()
            out_y(kind, way, k, mine).wait_send()
            out_d(kind, way, k, mine).wait_send()
            out_e(kind, way, k, across).wait_send()

        each_column(column_out)
        for k in range(steps):
            for way in (0, 1):

                @pl.when(leaves(way, k))
                def _():
                    out_z(way, k, carried(way, k)).wait_send()

    out_begin()
    w_first(0, 0).start()

    @pl.when(core == 0)
    def _():
        w_first(0, 1).start()
        w_first(0, 2).start()
        a1(0).start()
        a1(1).start()
        a2(0).start()
        w_first(1, 0).start()
        w_first(1, 1).start()
        a2(1).start()
        w_first(1, 2).start()

    @pl.when(core == 1)
    def _():
        a1(0).start()
        w_first(0, 1).start()
        a1(1).start()
        w_first(0, 2).start()
        w_first(1, 0).start()
        w_first(1, 1).start()
        w_first(1, 2).start()
        a2(0).start()
        a2(1).start()

    arr(0, 0)
    arr(0, 1)
    oz(1, 0)
    pas(0, 0)
    arr(1, 0)
    oz(0, 0)
    fwd(0)
    oe(0, 0, 0)
    arr(0, 2)
    pas(0, 1)
    oe(0, 1, 0)
    arr(1, 1)
    pas(1, 0)
    fwd(1)
    out_partner().start()
    begin_fv()
    pas(0, 2)
    arr(1, 2)
    near_dots()
    ox(0, 0)
    ox(1, 0)
    oe(1, 0, 0)
    arr(2, 0)
    oz(1, 1)
    pas(1, 2)
    oz(0, 1)
    arr(2, 1)
    oxp()
    pas(1, 1)
    oe(1, 1, 0)
    pas(2, 0)
    comb(0, 1)
    comb(0, 0)
    oe(0, 1, 1)
    oe(0, 0, 1)
    arr(2, 2)
    pas(2, 1)
    ox(1, 1)
    ox(0, 1)
    pas(2, 2)
    far_dots()
    row_dots(2, a2)
    oe(1, 0, 1)
    oz(0, 2)
    oe(1, 1, 1)
    oz(1, 2)
    comb(1, 1)
    comb(1, 0)
    row_dots(3, a3)
    comb(1, 3)
    comb(0, 3)
    oe(0, 1, 2)
    oe(0, 0, 2)
    ox(1, 2)
    comb(1, 2)
    comb(0, 2)
    ox(0, 2)
    attend()
    oe(1, 0, 2)
    oe(1, 1, 2)
    finish()
    drain()


def fused(local_rows, w3, out_weight, firsts, mix_table, mix_index, lengths, ranks):
    line = ranks // PAIR
    steps = line - 1
    own_rows, width = local_rows.shape
    head_width = w3.shape[2]
    half = width // PAIR
    kind = local_rows.dtype
    total_rows = ranks * own_rows
    dma = pltpu.SemaphoreType.DMA
    anywhere = pl.BlockSpec(memory_space=pltpu.HBM)
    scalars = pl.BlockSpec(memory_space=pltpu.SMEM)
    tile = (2, BLOCKS, 3, own_rows, head_width)
    return pl.pallas_call(
        functools.partial(whole_layer, line),
        out_shape=jax.ShapeDtypeStruct((own_rows, width), kind),
        in_specs=[anywhere] * 4 + [scalars] * 3,
        out_specs=pl.BlockSpec(memory_space=pltpu.VMEM),
        scratch_shapes=[
            pltpu.VMEM((BLOCKS * own_rows, half), kind),
            pltpu.VMEM((2, 3, half, 2 * head_width), kind),
            pltpu.VMEM((ranks * head_width, width), kind),
            pltpu.VMEM(tile, jnp.float32),
            pltpu.VMEM(tile, kind),
            pltpu.VMEM(tile, kind),
            pltpu.VMEM(tile[1:], kind),
            pltpu.VMEM((3, total_rows, head_width), kind),
            pltpu.VMEM((total_rows, head_width), kind),
            pltpu.VMEM((total_rows, head_width), kind),
            pltpu.VMEM((own_rows, ranks * head_width), kind),
            dma((4,)),
            dma((2, 3, 3)), dma((2, 3, 3)), dma((2, 3, 3)), dma((2, 3, 3)),
            dma((2, PIECES)), dma((2, PIECES)), dma((2, PIECES)),
            dma((2, 2, BLOCKS)), dma((2, BLOCKS)),
            dma((2, 2, steps)), dma((2, 3, steps)),
            dma((2, 2, 2, steps)), dma((2, 2, 2, steps)), dma((2, 2, 2, steps)),
            dma((2, ranks - 1)), dma((2, ranks - 1)),
        ],
        compiler_params=pltpu.CompilerParams(
            collective_id=0, has_side_effects=True, vmem_limit_bytes=60 * 1024 * 1024
        ),
    )(local_rows, w3, out_weight, firsts, mix_table, mix_index, lengths)


def body_fused(hidden_in, first_values, qkv_weight, out_weight, mix_table, mix_index, lengths):
    return fused(
        hidden_in[0], qkv_weight.transpose(1, 0, 2), out_weight, first_values[0],
        mix_table.T, mix_index, lengths, lax.axis_size("tensor"),
    )[None]


def chosen(hidden_in, first_values, qkv_weight, out_weight, mix_table, mix_index, lengths):
    args = (hidden_in, first_values, qkv_weight, out_weight, mix_table, mix_index, lengths)
    ranks = lax.axis_size("tensor")
    total_rows = ranks * hidden_in.shape[1]
    fits = ranks * out_weight.size * 2 <= total_rows * hidden_in.shape[2] * 4
    two = lax.axis_size("groups") == 2 and lax.axis_size("dp") == 2
    pairs = ranks == BLOCKS * PAIR and hidden_in.shape[2] % (SHARERS * PAIR * 128) == 0
    single = mix_index.shape[0] == 1 and qkv_weight.shape[2] == 128
    if fits and two and pairs and single:
        return body_fused(*args)
    return body(*args)


def solution(mesh):
    placed = (
        P(("groups", "dp"), "tensor", None),
        P(("groups", "dp"), "tensor", None),
        P(None, None, "tensor"),
        P("tensor", None),
        P(),
        P("tensor"),
        P(("groups", "dp")),
    )
    return jax.shard_map(
        chosen,
        mesh=mesh,
        in_specs=placed,
        out_specs=P(("groups", "dp"), "tensor", None),
        check_vma=False,
    )
```

```python
import functools
import math

import jax
import jax.numpy as jnp
from jax import lax
from jax.experimental import pallas as pl
from jax.experimental.pallas import tpu as pltpu
from jax.sharding import PartitionSpec as P

NEG_FILL = -1e30
PAIR = 2


def attention(queries, key_rows, mixed_values, valid_length, head_size):
    total_rows = queries.shape[0]
    positions = jnp.arange(total_rows, dtype=jnp.int32)
    score_scale = 1.0 / math.sqrt(head_size)
    block_rows = min(512, total_rows)
    outputs = []
    for first_row in range(0, total_rows, block_rows):
        stop = first_row + block_rows
        scores = (
            jnp.einsum(
                "qhd,khd->hqk",
                queries[first_row:stop],
                key_rows[:stop],
                preferred_element_type=jnp.float32,
            )
            * score_scale
        )
        keys_at, rows_at = positions[:stop], positions[first_row:stop]
        allowed = (keys_at[None, :] <= rows_at[:, None]) & (keys_at[None, :] < valid_length)
        scores = jnp.where(allowed[None], scores, NEG_FILL)
        row_max = jnp.max(scores, axis=2, keepdims=True)
        raised = jnp.exp(scores - row_max)
        weights = (raised / jnp.sum(raised, axis=2, keepdims=True)).astype(jnp.bfloat16)
        outputs.append(
            jnp.einsum(
                "hqk,khd->qhd", weights, mixed_values[:stop], preferred_element_type=jnp.float32
            ).astype(jnp.bfloat16)
        )
    return jnp.concatenate(outputs, axis=0)


def body(hidden_in, first_values, qkv_weight, out_weight, mix_table, mix_index, lengths):
    local_rows = hidden_in[0]
    own_rows, model_width = local_rows.shape
    head_width = qkv_weight.shape[2]
    heads_here = mix_index.shape[0]
    head_size = head_width // heads_here
    ranks = lax.axis_size("tensor")
    cores = lax.axis_size("dp")
    rank = lax.axis_index("tensor")
    core = lax.axis_index("dp")
    side = rank % PAIR
    line = ranks // PAIR
    swap_pair = [(r, r ^ 1) for r in range(ranks)]
    swap_core = [(c, c ^ 1) for c in range(cores)]

    own_w = qkv_weight.reshape(model_width, 3 * head_width)
    half = model_width // 2
    sent = lax.dynamic_slice_in_dim(own_w, core * half, half, 0)
    got = lax.ppermute(sent, "tensor", swap_pair)
    got_other = lax.ppermute(got, "dp", swap_core)
    pair_w = jnp.where(
        core == 0,
        jnp.concatenate([got, got_other], axis=0),
        jnp.concatenate([got_other, got], axis=0),
    )

    lines = [[s + PAIR * i for i in range(line)] for s in range(PAIR)]
    rows = lax.all_gather(local_rows, "tensor", axis=0, tiled=True, axis_index_groups=lines)
    for_pair = jnp.dot(rows, pair_w, preferred_element_type=jnp.float32).astype(jnp.bfloat16)
    from_pair = lax.ppermute(for_pair, "tensor", swap_pair)
    ours = jnp.dot(rows, own_w, preferred_element_type=jnp.float32).astype(jnp.bfloat16)
    ours = ours.reshape(line, own_rows, 3 * head_width)
    from_pair = from_pair.reshape(line, own_rows, 3 * head_width)
    projected = jnp.where(
        side == 0,
        jnp.stack([ours, from_pair], axis=1),
        jnp.stack([from_pair, ours], axis=1),
    )
    total_rows = ranks * own_rows
    split_parts = projected.reshape(total_rows, 3, heads_here, head_size)

    relaid = lax.all_to_all(first_values[0], "tensor", split_axis=1, concat_axis=0, tiled=True)
    firsts = relaid.reshape(total_rows, heads_here, head_size)
    levels = mix_table.shape[0]
    one_hot = (mix_index[:, None] == jnp.arange(levels, dtype=jnp.int32)[None, :]).astype(
        jnp.float32
    )
    weights_mix = jnp.dot(one_hot, mix_table, precision=lax.Precision.HIGHEST)
    mixed_values = (
        weights_mix[None, :, 0:1] * split_parts[:, 2].astype(jnp.float32)
        + weights_mix[None, :, 1:2] * firsts.astype(jnp.float32)
    ).astype(jnp.bfloat16)
    attended = attention(
        split_parts[:, 0], split_parts[:, 1], mixed_values, lengths[0], head_size
    ).reshape(total_rows, head_width)

    gathered_bytes = ranks * out_weight.size * 2
    summed_bytes = total_rows * model_width * 4
    if gathered_bytes > summed_bytes:
        kept_rows = lax.psum_scatter(
            jnp.dot(attended, out_weight, preferred_element_type=jnp.float32),
            "tensor",
            scatter_dimension=0,
            tiled=True,
        )
        return kept_rows.astype(jnp.bfloat16)[None]

    part = head_width // 2
    own_part = lax.dynamic_slice_in_dim(out_weight, core * part, part, 0)
    mine = lax.all_gather(own_part, "tensor", axis=0, tiled=True)
    other = lax.ppermute(mine, "dp", swap_core)
    kept = lax.all_to_all(attended, "tensor", split_axis=0, concat_axis=1, tiled=True)
    kept = kept.reshape(own_rows, ranks, 2, part)
    low = kept[:, :, 0].reshape(own_rows, ranks * part)
    high = kept[:, :, 1].reshape(own_rows, ranks * part)
    out = jnp.dot(
        jnp.where(core == 0, low, high), mine, preferred_element_type=jnp.float32
    ) + jnp.dot(jnp.where(core == 0, high, low), other, preferred_element_type=jnp.float32)
    return out.astype(jnp.bfloat16)[None]


PIECES = 2
SHARERS = 4
BLOCKS = 4
MESH = pl.DeviceIdType.MESH


def whole_layer(
    line, rows_ref, w_ref, ow_ref, fv_ref, table_ref, index_ref, length_ref, out_ref,
    hid, wts, wf_ref, kept, px_out, px_in, finished, qkv_ref, fo_ref, att, gathered_att, levels,
    load_sem, w_sem, wy_sem, wd_sem, we_sem, a1_sem, a2_sem, a3_sem, cx_sem, cz_sem,
    oz_sem, ox_sem, oy_sem, od_sem, oe_sem, fv_sem, at_sem,
):
    group, core, rank = lax.axis_index("groups"), lax.axis_index("dp"), lax.axis_index("tensor")
    spot, side = rank // PAIR, rank % PAIR
    ranks = line * PAIR
    steps = line - 1
    own_rows, width = rows_ref.shape
    half = width // PAIR
    part = half // SHARERS
    head = w_ref.shape[2]
    piece = own_rows // PIECES
    quarter = head // SHARERS
    mine, across = group * 2 + core, (1 - group) * 2 + core
    sib_mine, sib_across = group * 2 + 1 - core, (1 - group) * 2 + 1 - core
    near = spot + 1 - 2 * (spot % 2)
    far = (spot + line // 2) % line
    left, right = (group, core, rank - PAIR), (group, core, rank + PAIR)
    partner = (group, core, spot * PAIR + 1 - side)
    rows_peer = (group, core, far * PAIR + side)
    heads_peer = (group, core, near * PAIR + side)
    opposite = (1 - group, core, rank)
    sibling = (group, 1 - core, rank)
    has_left, has_right = spot > 0, spot < steps

    barrier = pltpu.get_barrier_semaphore()
    peers = [(group, core, (rank + o) % ranks) for o in range(1, ranks)]
    for there in peers + [opposite, sibling]:
        pl.semaphore_signal(barrier, inc=1, device_id=there, device_id_type=MESH)

    def cut(index, size):
        return pl.ds(pl.multiple_of(index * size, size), size)

    def row_block(b, p=None):
        if p is None:
            return pl.ds(b * own_rows, own_rows)
        return pl.ds(b * own_rows + p * piece, piece)

    own_half, other_half = cut(side, half), cut(1 - side, half)
    loads = [
        pltpu.make_async_copy(rows_ref.at[:, own_half], hid.at[row_block(0), :], load_sem.at[0]),
        pltpu.make_async_copy(w_ref.at[:, own_half, :], wts.at[0, :, :, pl.ds(0, head)], load_sem.at[1]),
        pltpu.make_async_copy(ow_ref, wf_ref.at[cut(rank, head), :], load_sem.at[2]),
        pltpu.make_async_copy(fv_ref.at[:, cut(rank, head)], fo_ref.at[cut(rank, own_rows), :], load_sem.at[3]),
        pltpu.make_async_copy(table_ref, levels, load_sem.at[4]),
    ]
    for load in loads:
        load.start()
    pl.semaphore_wait(barrier, ranks + 1)

    def send(src, dst, sems, at, there):
        return pltpu.make_async_remote_copy(
            src_ref=src, dst_ref=dst, send_sem=sems.at[(0,) + at], recv_sem=sems.at[(1,) + at],
            device_id=there, device_id_type=MESH,
        )

    def wpart(kind, j, q):
        zone, lane = (0, 1) if kind == 0 else (1, kind - 1)
        return wts.at[zone, j, cut(q, part), pl.ds(lane * head, head)]

    def w_source(s, j):
        return w_ref.at[j, pl.ds(pl.multiple_of(s * half + mine * part, part), part), :]

    def w_first(kind, j):
        if kind == 0:
            return send(w_source(1 - side, j), wpart(0, j, mine), w_sem, (0, j), partner)
        source = w_source(side, j) if kind == 1 else wpart(0, j, mine)
        return send(source, wpart(kind, j, mine), w_sem, (kind, j), heads_peer)

    def w_across(kind, j, q):
        return send(wpart(kind, j, q), wpart(kind, j, q), wy_sem, (kind, j), opposite)

    def w_down(kind, j, q):
        return send(wpart(kind, j, q), wpart(kind, j, q), wd_sem, (kind, j), sibling)

    def w_echo(kind, j, q):
        return send(wpart(kind, j, q), wpart(kind, j, q), we_sem, (kind, j), sibling)

    def arr(kind, j):
        w_first(kind, j).wait_recv()
        if kind == 0:
            w_first(2, j).start()
        w_across(kind, j, mine).start()
        w_down(kind, j, mine).start()

    def pas(kind, j):
        w_across(kind, j, across).wait_recv()
        w_echo(kind, j, across).start()

    def w_ready(kind):
        for j in range(3):
            w_down(kind, j, sib_mine).wait_recv()
            w_echo(kind, j, sib_across).wait_recv()

    def a1(p):
        return send(
            rows_ref.at[pl.ds(p * piece, piece), other_half], hid.at[row_block(1, p), :], a1_sem, (p,), partner
        )

    def a2(p):
        return send(
            rows_ref.at[pl.ds(p * piece, piece), own_half], hid.at[row_block(2, p), :], a2_sem, (p,), rows_peer
        )

    def a3(p):
        return send(hid.at[row_block(1, p), :], hid.at[row_block(3, p), :], a3_sem, (p,), rows_peer)

    def fwd(p):
        a1(p).wait_recv()
        a3(p).start()

    def swapped(b):
        return b + 1 - 2 * (b % 2)

    def cx(e, b):
        return pltpu.make_async_remote_copy(
            src_ref=px_out.at[e, b], dst_ref=px_in.at[e, swapped(b)], send_sem=cx_sem.at[0, e, b],
            recv_sem=cx_sem.at[1, e, swapped(b)], device_id=partner, device_id_type=MESH,
        )

    def place(b):
        return cut((spot, far)[b // 2] * PAIR + (side, 1 - side)[b % 2], own_rows)

    def cz(b):
        return send(finished.at[b], qkv_ref.at[:, place(b), :], cz_sem, (b,), heads_peer)

    def project(e, first, count):
        def one(j, carry):
            total = jnp.dot(
                hid[pl.ds(first * own_rows, count * own_rows), :], wts[e, j],
                preferred_element_type=jnp.float32,
            )
            for i in range(count):
                rows = total[i * own_rows : (i + 1) * own_rows]
                kept[e, first + i, j] = rows[:, :head]
                px_out[e, first + i, j] = rows[:, head:].astype(jnp.bfloat16)
            return carry

        lax.fori_loop(0, 3, one, 0)
        for b in range(first, first + count):
            cx(e, b).start()

    def comb(e, b):
        cx(e, swapped(b)).wait_recv()
        total = (kept[e, b] + px_in[e, b].astype(jnp.float32)).astype(jnp.bfloat16)
        if e == 0:
            qkv_ref[:, place(b), :] = total
        else:
            finished[b] = total
            cz(b).start()

    def first_copy(o):
        return send(fv_ref.at[:, cut(peers[o][2], head)], fo_ref.at[cut(rank, own_rows), :], fv_sem, (o,), peers[o])

    def wf(column, q):
        return wf_ref.at[pl.ds(pl.multiple_of(column * head + q * quarter, quarter), quarter), :]

    def wf_half(column, c):
        return wf_ref.at[pl.ds(pl.multiple_of(column * head + c * (head // 2), head // 2), head // 2), :]

    def chunk(way, k):
        return spot - 1 - k if way == 0 else spot + 1 + k

    def arrives(way, k):
        return k < spot if way == 0 else spot + 1 + k < line

    def leaves(way, k):
        if way == 0:
            return jnp.logical_and(k <= spot, has_right)
        return jnp.logical_and(spot + k < line, has_left)

    def carried(way, k):
        return spot - k if way == 0 else spot + k

    def column_of(kind, way, k):
        at = chunk(way, k)
        return at * PAIR + (side if kind == 0 else 1 - side)

    def out_z(way, k, at):
        column = at * PAIR + side
        source = ow_ref.at[cut(mine, quarter), :] if k == 0 else wf(column, mine)
        return send(source, wf(column, mine), oz_sem, (way, k), right if way == 0 else left)

    def out_x(way, k, column):
        return send(wf(column, mine), wf(column, mine), ox_sem, (way, k), partner)

    def out_y(kind, way, k, q):
        column = column_of(kind, way, k)
        return send(wf(column, q), wf(column, q), oy_sem, (kind, way, k), opposite)

    def out_d(kind, way, k, q):
        column = column_of(kind, way, k)
        return send(wf(column, q), wf(column, q), od_sem, (kind, way, k), sibling)

    def out_e(kind, way, k, q):
        column = column_of(kind, way, k)
        return send(wf(column, q), wf(column, q), oe_sem, (kind, way, k), sibling)

    partner_column = spot * PAIR + 1 - side

    def out_partner():
        return send(ow_ref.at[cut(core, head // 2), :], wf_half(rank, core), ox_sem, (2, 0), partner)

    def out_shared(c):
        return send(wf_half(partner_column, c), wf_half(partner_column, c), ox_sem, (2, 1), sibling)

    def oxp():
        out_partner().wait_recv()
        out_shared(core).start()

    def out_begin():
        for way in (0, 1):

            @pl.when(leaves(way, 0))
            def _():
                out_z(way, 0, spot).start()

    def oz(way, k):
        @pl.when(arrives(way, k))
        def _():
            at = chunk(way, k)
            out_z(way, k, at).wait_recv()
            if k + 1 < steps:

                @pl.when(leaves(way, k + 1))
                def _():
                    out_z(way, k + 1, at).start()

            out_x(way, k, column_of(0, way, k)).start()
            out_y(0, way, k, mine).start()
            out_d(0, way, k, mine).start()

    def ox(way, k):
        @pl.when(arrives(way, k))
        def _():
            out_x(way, k, column_of(1, way, k)).wait_recv()
            out_y(1, way, k, mine).start()
            out_d(1, way, k, mine).start()

    def oe(kind, way, k):
        @pl.when(arrives(way, k))
        def _():
            out_y(kind, way, k, across).wait_recv()
            out_e(kind, way, k, across).start()

    def begin_fv():
        for o in range(ranks - 1):
            first_copy(o).start()

    def near_dots():
        for load in loads:
            load.wait()
        w_ready(0)
        project(0, 0, 2)

    def row_dots():
        for p in range(PIECES):
            a2(p).wait_recv()
        project(0, 2, 1)

    def far_dots():
        w_ready(1)
        w_ready(2)
        project(1, 0, 3)

    def last_dots():
        for p in range(PIECES):
            a3(p).wait_recv()
        project(1, 3, 1)
        project(0, 3, 1)

    total_rows = ranks * own_rows
    block_rows = PAIR * own_rows

    def att_copy(r):
        return pltpu.make_async_remote_copy(
            src_ref=att.at[pl.ds(r * own_rows, own_rows), :], dst_ref=gathered_att.at[:, cut(rank, head)],
            send_sem=at_sem.at[0, r], recv_sem=at_sem.at[1, rank], device_id=(group, core, r), device_id_type=MESH,
        )

    def att_arrival(r):
        return pltpu.make_async_remote_copy(
            src_ref=att.at[pl.ds(r * own_rows, own_rows), :],
            dst_ref=gathered_att.at[:, pl.ds(r * head, head)],
            send_sem=at_sem.at[0, r], recv_sem=at_sem.at[1, r], device_id=(group, core, r), device_id_type=MESH,
        )

    def att_own():
        return pltpu.make_async_copy(
            att.at[cut(rank, own_rows), :], gathered_att.at[:, cut(rank, head)], load_sem.at[0]
        )

    def others(action):
        for r in range(ranks):

            @pl.when(rank != r)
            def _():
                action(r)

    def attend():
        for b in range(BLOCKS):
            cz(b).wait_recv()
        for o in range(ranks - 1):
            first_copy(o).wait_recv()
        chosen_row = index_ref[0]
        now, before = levels[0, chosen_row], levels[1, chosen_row]
        valid = length_ref[0]
        values = (now * qkv_ref[2].astype(jnp.float32) + before * fo_ref[...].astype(jnp.float32)).astype(
            jnp.bfloat16
        )
        score_scale = 1.0 / math.sqrt(head)
        for first_row in range(0, total_rows, block_rows):
            stop = first_row + block_rows
            scores = lax.dot_general(
                qkv_ref[0, first_row:stop, :], qkv_ref[1, :stop, :], (((1,), (1,)), ((), ())),
                preferred_element_type=jnp.float32,
            ) * score_scale
            shape = (block_rows, stop)
            limit = jnp.minimum(lax.broadcasted_iota(jnp.int32, (block_rows, 1), 0) + (first_row + 1), valid)
            scores = jnp.where(lax.broadcasted_iota(jnp.int32, shape, 1) < limit, scores, NEG_FILL)
            raised = jnp.exp(scores - jnp.max(scores, axis=1, keepdims=True))
            weights = (raised / jnp.sum(raised, axis=1, keepdims=True)).astype(jnp.bfloat16)
            att[first_row:stop, :] = jnp.dot(
                weights, values[:stop], preferred_element_type=jnp.float32
            ).astype(jnp.bfloat16)
            for r in range(first_row // own_rows, stop // own_rows):

                @pl.when(rank != r)
                def _():
                    att_copy(r).start()

        att_own().start()

    def each_column(action):
        for k in range(steps):
            for way in (0, 1):

                @pl.when(arrives(way, k))
                def _():
                    for kind in (0, 1):
                        action(kind, way, k)

    def column_in(kind, way, k):
        out_d(kind, way, k, sib_mine).wait_recv()
        out_e(kind, way, k, sib_across).wait_recv()

    def finish():
        att_own().wait()
        others(lambda r: att_arrival(r).wait_recv())
        each_column(column_in)
        out_shared(1 - core).wait_recv()
        wide = width // (2 * PIECES * PAIR) if width % (1024 * PIECES) == 0 else width

        def one(i, carry):
            at = pl.ds(pl.multiple_of(i * wide, wide), wide)
            out_ref[:, at] = jnp.dot(
                gathered_att[...], wf_ref[:, at], preferred_element_type=jnp.float32
            ).astype(jnp.bfloat16)
            return carry

        lax.fori_loop(0, width // wide, one, 0)

    def drain():
        for p in range(PIECES):
            a1(p).wait_send()
            a2(p).wait_send()
            a3(p).wait_send()
        for kind in range(3):
            for j in range(3):
                w_first(kind, j).wait_send()
                w_across(kind, j, mine).wait_send()
                w_down(kind, j, mine).wait_send()
                w_echo(kind, j, across).wait_send()
        for e in range(2):
            for b in range(BLOCKS):
                cx(e, b).wait_send()
        for b in range(BLOCKS):
            cz(b).wait_send()
        for o in range(ranks - 1):
            first_copy(o).wait_send()
        others(lambda r: att_copy(r).wait_send())
        out_partner().wait_send()
        out_shared(core).wait_send()

        def column_out(kind, way, k):
            if kind == 0:
                out_x(way, k, column_of(0, way, k)).wait_send()
            out_y(kind, way, k, mine).wait_send()
            out_d(kind, way, k, mine).wait_send()
            out_e(kind, way, k, across).wait_send()

        each_column(column_out)
        for k in range(steps):
            for way in (0, 1):

                @pl.when(leaves(way, k))
                def _():
                    out_z(way, k, carried(way, k)).wait_send()

    ends = jnp.logical_or(spot == 0, spot == steps)
    places = [
        jnp.logical_and(ends, core == 0), jnp.logical_and(ends, core == 1),
        jnp.logical_and(jnp.logical_not(ends), core == 0), jnp.logical_and(jnp.logical_not(ends), core == 1),
    ]

    @pl.when(places[0])
    def _():
        w_first(0, 0).start()
        w_first(0, 1).start()
        w_first(0, 2).start()
        a1(0).start()
        a1(1).start()
        out_begin()
        w_first(1, 0).start()
        w_first(1, 1).start()
        w_first(1, 2).start()
        a2(0).start()
        a2(1).start()
        arr(0, 0)
        arr(0, 1)
        oz(0, 0)
        oz(1, 0)
        arr(0, 2)
        out_partner().start()
        pas(0, 1)
        arr(1, 0)
        fwd(0)
        pas(0, 0)
        oe(0, 0, 0)
        arr(1, 1)
        oe(0, 1, 0)
        fwd(1)
        pas(0, 2)
        arr(1, 2)
        pas(1, 1)
        pas(1, 0)
        ox(1, 0)

    @pl.when(places[1])
    def _():
        a1(0).start()
        w_first(0, 0).start()
        a1(1).start()
        w_first(0, 1).start()
        w_first(0, 2).start()
        out_begin()
        a2(0).start()
        w_first(1, 0).start()
        w_first(1, 1).start()
        w_first(1, 2).start()
        a2(1).start()
        arr(0, 0)
        oz(0, 0)
        pas(0, 0)
        oz(1, 0)
        fwd(0)
        oe(0, 0, 0)
        arr(1, 0)
        arr(0, 1)
        oe(0, 1, 0)
        arr(0, 2)
        out_partner().start()
        pas(1, 0)
        arr(1, 1)
        pas(0, 1)
        fwd(1)
        pas(0, 2)

    @pl.when(places[2])
    def _():
        w_first(0, 0).start()
        w_first(0, 1).start()
        a1(0).start()
        a1(1).start()
        w_first(0, 2).start()
        out_begin()
        w_first(1, 0).start()
        w_first(1, 1).start()
        w_first(1, 2).start()
        a2(0).start()
        a2(1).start()
        arr(0, 0)
        oz(1, 0)
        oz(0, 0)
        arr(0, 1)
        pas(0, 0)
        arr(1, 0)
        fwd(0)
        arr(1, 1)
        fwd(1)
        oe(0, 0, 0)
        pas(0, 1)
        arr(0, 2)
        out_partner().start()
        oe(0, 1, 0)
        pas(1, 1)
        pas(1, 0)
        ox(0, 0)
        pas(0, 2)
        ox(1, 0)
        arr(1, 2)

    @pl.when(places[3])
    def _():
        w_first(0, 0).start()
        a1(0).start()
        w_first(0, 1).start()
        a1(1).start()
        w_first(0, 2).start()
        out_begin()
        w_first(1, 0).start()
        w_first(1, 1).start()
        a2(0).start()
        a2(1).start()
        w_first(1, 2).start()
        arr(0, 0)
        oz(1, 0)
        arr(0, 1)
        arr(1, 1)
        oz(0, 0)
        pas(0, 0)
        fwd(0)
        arr(1, 0)
        arr(1, 2)
        arr(0, 2)
        out_partner().start()
        pas(0, 1)
        oe(0, 1, 0)
        fwd(1)
        oe(0, 0, 0)
        pas(1, 0)
        pas(1, 1)
        ox(1, 0)
        pas(1, 2)
        pas(0, 2)
        ox(0, 0)

    near_dots()

    @pl.when(places[0])
    def _():
        pas(1, 2)
        arr(2, 0)

    @pl.when(places[1])
    def _():
        pas(1, 1)
        arr(1, 2)
        ox(0, 0)
        ox(1, 0)
        arr(2, 0)
        pas(1, 2)

    row_dots()

    @pl.when(places[0])
    def _():
        oe(1, 1, 0)
        ox(0, 0)
        oe(1, 0, 0)
        pas(2, 0)
        oz(1, 1)
        arr(2, 1)
        oz(0, 1)
        oxp()
        pas(2, 1)
        comb(0, 1)
        oe(0, 1, 1)
        comb(0, 0)
        oe(0, 0, 1)
        arr(2, 2)
        begin_fv()
        pas(2, 2)

    @pl.when(places[1])
    def _():
        oe(1, 0, 0)
        oe(1, 1, 0)
        pas(2, 0)
        arr(2, 1)
        oz(1, 1)
        oxp()
        oz(0, 1)
        pas(2, 1)
        oe(0, 1, 1)
        comb(0, 0)
        oe(0, 0, 1)
        arr(2, 2)
        begin_fv()
        pas(2, 2)
        oz(0, 2)
        ox(0, 1)

    @pl.when(places[2])
    def _():
        oz(1, 1)
        arr(2, 1)
        arr(2, 0)
        arr(2, 2)
        begin_fv()
        oz(0, 1)
        oe(1, 1, 0)
        pas(1, 2)
        oxp()
        pas(2, 1)
        pas(2, 0)
        oe(1, 0, 0)
        comb(0, 1)
        comb(0, 0)
        pas(2, 2)
        ox(1, 1)
        oe(0, 1, 1)
        ox(0, 1)
        oe(0, 0, 1)

    @pl.when(places[3])
    def _():
        oz(1, 1)
        arr(2, 0)
        oe(1, 1, 0)
        oz(0, 1)
        oe(1, 0, 0)
        oxp()
        comb(0, 1)
        pas(2, 0)
        comb(0, 0)
        arr(2, 1)
        oe(0, 0, 1)
        arr(2, 2)
        begin_fv()
        pas(2, 1)
        oe(0, 1, 1)
        ox(0, 1)
        pas(2, 2)

    far_dots()

    @pl.when(places[0])
    def _():
        ox(0, 1)
        ox(1, 1)
        comb(1, 1)
        comb(1, 0)
        oz(0, 2)
        oe(1, 1, 1)
        oz(1, 2)
        oe(1, 0, 1)

    @pl.when(places[1])
    def _():
        ox(1, 1)
        comb(1, 1)
        comb(1, 0)
        oe(1, 0, 1)
        oe(1, 1, 1)
        comb(0, 1)
        oz(1, 2)

    @pl.when(places[3])
    def _():
        ox(1, 1)
        comb(1, 1)

    last_dots()

    @pl.when(places[0])
    def _():
        comb(1, 3)
        comb(0, 3)
        oe(0, 1, 2)
        ox(0, 2)
        comb(1, 2)
        oe(0, 0, 2)
        ox(1, 2)
        comb(0, 2)
        oe(1, 0, 2)

    @pl.when(places[1])
    def _():
        oe(0, 0, 2)
        ox(0, 2)
        comb(0, 3)
        comb(1, 3)
        oe(0, 1, 2)
        ox(1, 2)
        comb(1, 2)
        comb(0, 2)
        oe(1, 1, 2)

    @pl.when(places[2])
    def _():
        oe(1, 0, 1)
        comb(1, 1)
        oe(1, 1, 1)
        comb(1, 0)
        comb(1, 3)
        comb(0, 3)
        comb(1, 2)
        comb(0, 2)

    @pl.when(places[3])
    def _():
        comb(0, 3)
        comb(1, 0)
        oe(1, 0, 1)
        comb(1, 3)
        oe(1, 1, 1)
        comb(1, 2)
        comb(0, 2)

    attend()

    @pl.when(places[0])
    def _():
        oe(1, 1, 2)

    @pl.when(places[1])
    def _():
        oe(1, 0, 2)

    finish()
    drain()


def fused(local_rows, w3, out_weight, firsts, mix_table, mix_index, lengths, ranks):
    line = ranks // PAIR
    steps = line - 1
    own_rows, width = local_rows.shape
    head_width = w3.shape[2]
    half = width // PAIR
    kind = local_rows.dtype
    total_rows = ranks * own_rows
    dma = pltpu.SemaphoreType.DMA
    anywhere = pl.BlockSpec(memory_space=pltpu.HBM)
    scalars = pl.BlockSpec(memory_space=pltpu.SMEM)
    tile = (2, BLOCKS, 3, own_rows, head_width)
    held = (local_rows, w3, out_weight, firsts, mix_table)
    return pl.pallas_call(
        functools.partial(whole_layer, line),
        out_shape=jax.ShapeDtypeStruct((own_rows, width), kind),
        in_specs=[anywhere] * 5 + [scalars] * 2,
        out_specs=pl.BlockSpec(memory_space=pltpu.VMEM),
        scratch_shapes=[
            pltpu.VMEM((BLOCKS * own_rows, half), kind),
            pltpu.VMEM((2, 3, half, 2 * head_width), kind),
            pltpu.VMEM((ranks * head_width, width), kind),
            pltpu.VMEM(tile, jnp.float32),
            pltpu.VMEM(tile, kind),
            pltpu.VMEM(tile, kind),
            pltpu.VMEM(tile[1:], kind),
            pltpu.VMEM((3, total_rows, head_width), kind),
            pltpu.VMEM((total_rows, head_width), kind),
            pltpu.VMEM((total_rows, head_width), kind),
            pltpu.VMEM((own_rows, ranks * head_width), kind),
            pltpu.SMEM(mix_table.shape, mix_table.dtype),
            dma((5,)),
            dma((2, 3, 3)), dma((2, 3, 3)), dma((2, 3, 3)), dma((2, 3, 3)),
            dma((2, PIECES)), dma((2, PIECES)), dma((2, PIECES)),
            dma((2, 2, BLOCKS)), dma((2, BLOCKS)),
            dma((2, 2, steps)), dma((2, 3, steps)),
            dma((2, 2, 2, steps)), dma((2, 2, 2, steps)), dma((2, 2, 2, steps)),
            dma((2, ranks - 1)), dma((2, ranks)),
        ],
        compiler_params=pltpu.CompilerParams(
            collective_id=0, has_side_effects=True, vmem_limit_bytes=52 * 1024 * 1024
        ),
    )(*[pltpu.with_memory_space_constraint(a, pltpu.HBM) for a in held], mix_index, lengths)


def body_fused(hidden_in, first_values, qkv_weight, out_weight, mix_table, mix_index, lengths):
    return fused(
        hidden_in[0], qkv_weight.transpose(1, 0, 2), out_weight, first_values[0],
        mix_table.T, mix_index, lengths, lax.axis_size("tensor"),
    )[None]


def chosen(hidden_in, first_values, qkv_weight, out_weight, mix_table, mix_index, lengths):
    args = (hidden_in, first_values, qkv_weight, out_weight, mix_table, mix_index, lengths)
    ranks = lax.axis_size("tensor")
    total_rows = ranks * hidden_in.shape[1]
    fits = ranks * out_weight.size * 2 <= total_rows * hidden_in.shape[2] * 4
    two = lax.axis_size("groups") == 2 and lax.axis_size("dp") == 2
    pairs = ranks == BLOCKS * PAIR and hidden_in.shape[2] % (SHARERS * PAIR * 128) == 0
    single = mix_index.shape[0] == 1 and qkv_weight.shape[2] == 128
    if fits and two and pairs and single:
        return body_fused(*args)
    return body(*args)


def solution(mesh):
    placed = (
        P(("groups", "dp"), "tensor", None),
        P(("groups", "dp"), "tensor", None),
        P(None, None, "tensor"),
        P("tensor", None),
        P(),
        P("tensor"),
        P(("groups", "dp")),
    )
    return jax.shard_map(
        chosen,
        mesh=mesh,
        in_specs=placed,
        out_specs=P(("groups", "dp"), "tensor", None),
        check_vma=False,
    )
```
